32 devices in a mesh: grp: 2 (over y), exp: 4 (over z), tp: 4 (over x, core).
Axes of the slice: x: 2, y: 2, z: 4, core: 2. Of those that a mesh axis runs over, the one named last changes fastest.
Arguments:
- tokens: bfloat16 [128, 3584], P(('grp', 'exp'), 'tp'), parts along dimension 0, may hold values from -6 to 6
- gate_up_weight: bfloat16 [3584, 2, 18944], P('tp', None, 'exp'), may hold values from -0.09375 to 0.09375
- down_weight: bfloat16 [18944, 3584], P('exp', 'tp'), may hold values from -0.046875 to 0.046875
- adapter_in: bfloat16 [4, 3584, 16], P('exp', 'tp'), may hold values from -0.09375 to 0.09375
- adapter_out: bfloat16 [4, 16, 3584], P('exp', None, 'tp'), may hold values from -1.5 to 1.5
- expert_ids: int32 [128, 2], P(('grp', 'exp')), parts along dimension 0, may hold values from 0 to 3, all different within a row; in each aligned block of 16 rows (0 to 15, 16 to 31, ...) at most 16 rows name the same one
- route_weight: float32 [128, 2], P(('grp', 'exp')), parts along dimension 0, may hold values from 0.2 to 1
Outputs:
- mixed: bfloat16 [128, 3584], P(('grp', 'exp'), 'tp'), parts along dimension 0
The draws below stay inside these ranges and needn't reach their ends.
There are 2 independent parts, one for each index of `grp`. The reference program is written for one: setup_inputs(seed, part) draws one part's arguments, and reference() takes and returns one part's arrays. A program takes and returns all parts, laid end to end along the dimension named above; an argument that names none is the same for every part. Nothing has to cross between parts.
Inputs may be any that keep to these rules, and one draw needn't show every extreme that they name: `expert_ids`: each row names 2 different experts. Among the 16 rows of one index of exp (aligned blocks of 16 rows) no expert is named by more than 16 rows, and in every draw some expert is named by exactly 16 rows of some block.
All inputs are finite; a program needn't handle non-finite values.
Results may differ from the reference program's by a relative error of at most 0.025.
Values may be sent and summed in bfloat16 or wider, within the bound.
No kernel may reach another device: no remote copies, remote signals or barrier semaphores. Data moves between devices by JAX's collectives and lax.ppermute only.
A program may use at most 64 MiB of HBM per device.

```python
import math
import jax
import jax.numpy as jnp
import numpy as np
from jax import lax

D = 3584
FF = 18944
RANK = 16
TOP = 2
TOK_DEV = 16
EXPERTS = 4
TOKENS = 64
CAP = 16
N_EXP = 4
N_TP = 4


def steps_of(key, dims, cuts, least, top_value):
    level, own = 1.0, jax.random.fold_in(key, 6)
    for dim, shards_of in cuts:
        heights = jnp.exp(jax.random.uniform(jax.random.fold_in(own, dim), (shards_of,), jnp.float32, least / len(cuts), top_value / len(cuts)))
        level = level * jnp.repeat(heights, dims[dim] // shards_of).reshape([-1 if axis == dim else 1 for axis in range(len(dims))])
    return level


def assign_block(key, own, number, rows, count, top, reach, skew):
    sequence = jax.random.permutation(key, count)
    crowded, common = portions_of(count, rows * top, reach, skew, True), portions_of(count, rows * top, reach, skew, False)
    places = jnp.arange(count)

    def named(lengths, turn):
        used = int((lengths > 0).sum())
        fixed = max(1, used // 4)
        shifted = fixed + (places - fixed + turn * (used - fixed)) % max(1, count - fixed)
        return jnp.zeros((count,), jnp.int32).at[sequence[jnp.where(places < fixed, places, shifted)]].set(jnp.asarray(lengths, jnp.int32))

    lengths = jnp.where(number % 4 == 0, named(crowded, number // 4), named(common, number - number // 4 - 1))
    mixed = jax.random.permutation(jax.random.fold_in(own, 3), count)
    donor, taker = mixed[0:count // 2 * 2:2], mixed[1:count // 2 * 2:2]
    margin = jnp.minimum(lengths[donor] - 1, reach - lengths[taker]) // 2
    margin = jnp.where((donor == sequence[0]) | (taker == sequence[0]) | (lengths[taker] == 0), 0, jnp.maximum(margin, 0))
    shifted = jax.random.randint(jax.random.fold_in(own, 4), (count // 2,), 0, 1 << 20) % (margin + 1)
    lengths = lengths.at[donor].add(-shifted).at[taker].add(shifted)
    members = jnp.searchsorted(jnp.cumsum(lengths), jnp.arange(rows * top), side="right").astype(jnp.int32)
    listing = members.reshape(top, rows).T
    listing = listing[jax.random.permutation(jax.random.fold_in(own, 1), rows)]
    turn = jax.random.randint(jax.random.fold_in(own, 2), (rows, 1), 0, top)
    return jnp.take_along_axis(listing, (jnp.arange(top)[None, :] + turn) % top, axis=1)


def portions_of(count, total, bound, slope, full):
    portions = [(1 << 20) // math.isqrt(rank ** slope) + 1 for rank in range(1, count + 1)]
    largest = bound if full else min(bound, max(-(-total // count), total * portions[0] // sum(portions)))
    least = 1 if total - largest >= count - 1 else 0
    holding, spare = [largest] + [least] * (count - 1), total - largest - least * (count - 1)
    while spare > 0:
        candidates = [i for i in range(1, count) if holding[i] < largest] or [i for i in range(1, count) if holding[i] < bound]
        whole, remaining = sum([portions[i] for i in candidates]), spare
        for i in candidates:
            more = min(bound - holding[i], max(1, remaining * portions[i] // whole), spare)
            holding[i] = holding[i] + more
            spare = spare - more
    return np.array(holding)


def scatter_about(own_key, shape, width, most, cuts=(), kind=jnp.bfloat16):
    level = steps_of(own_key, shape, cuts, -0.22, 0.18) if cuts else 1.0
    result = jax.random.normal(own_key, shape, jnp.float32) * width * level
    return jnp.minimum(jnp.maximum(result, -most), most).astype(kind)


def setup_inputs(seed: int = 0, part: int = 0) -> dict:
    keys = jax.random.split(jax.random.key(seed), 8)
    part_splits = jax.random.split(jax.random.fold_in(keys[7], part), 8)
    tokens = scatter_about(part_splits[0], (TOKENS, D), 1.0, 6.0, ((0, 4), (1, 4)))
    gate_up_weight = scatter_about(keys[1], (D, 2, FF), D ** -0.5, 0.09375, ((0, 4), (2, 4)))
    down_weight = scatter_about(keys[2], (FF, D), FF ** -0.5, 0.046875, ((0, 4), (1, 4)))
    adapter_in = scatter_about(keys[3], (EXPERTS, D, RANK), D ** -0.5, 0.09375, ((0, 4), (1, 4)))
    adapter_out = scatter_about(keys[4], (EXPERTS, RANK, D), RANK ** -0.5, 1.5, ((0, 4), (2, 4)))
    expert_ids_keys = jax.random.split(jax.random.fold_in(part_splits[5], 1), TOKENS // TOK_DEV)
    expert_ids_turns = jax.random.permutation(jax.random.fold_in(part_splits[5], 3), TOKENS // TOK_DEV)
    expert_ids = jax.vmap(lambda own, number: assign_block(jax.random.fold_in(part_splits[5], 2), own, number, TOK_DEV, EXPERTS, TOP, CAP, 2))(expert_ids_keys, expert_ids_turns).reshape((TOKENS, TOP))
    route_weight = jnp.clip(0.2 + 0.8 * jax.random.uniform(part_splits[6], (TOKENS, TOP), jnp.float32) ** steps_of(part_splits[6], (TOKENS, TOP), ((0, 4),), -0.2, 0.2), 0.2, 1.0)
    return dict(tokens=tokens, gate_up_weight=gate_up_weight, down_weight=down_weight, adapter_in=adapter_in, adapter_out=adapter_out, expert_ids=expert_ids, route_weight=route_weight)


def reference(tokens, gate_up_weight, down_weight, adapter_in, adapter_out, expert_ids, route_weight):
    token_count = tokens.shape[0]
    feat_width = D // N_TP
    pair = jnp.zeros((token_count, 2 * FF), jnp.float32)
    for block_index in range(N_TP):
        lower = block_index * feat_width
        block_weight = gate_up_weight[lower:lower + feat_width].reshape(feat_width, 2 * FF)
        partial_sum = jnp.dot(tokens[:, lower:lower + feat_width], block_weight, preferred_element_type=jnp.float32)
        rounded = lax.optimization_barrier(partial_sum.astype(jnp.bfloat16))
        pair = pair + rounded.astype(jnp.float32)
    gate = pair[:, :FF]
    up_part = pair[:, FF:]
    hidden = (jax.nn.silu(gate) * up_part).astype(jnp.bfloat16)
    hidden_width = FF // N_EXP
    base_out = jnp.zeros((token_count, D), jnp.float32)
    for block_index in range(N_EXP):
        lower = block_index * hidden_width
        partial_sum = jnp.dot(hidden[:, lower:lower + hidden_width], down_weight[lower:lower + hidden_width], preferred_element_type=jnp.float32)
        rounded = lax.optimization_barrier(partial_sum.astype(jnp.bfloat16))
        base_out = base_out + rounded.astype(jnp.float32)
    expert_count = adapter_in.shape[0]
    in_flat = jnp.transpose(adapter_in, (1, 0, 2)).reshape(D, expert_count * RANK)
    rank_mid = jnp.dot(tokens, in_flat, preferred_element_type=jnp.float32).astype(jnp.bfloat16)
    rank_mid = rank_mid.reshape(token_count, expert_count, RANK)
    hits = (expert_ids[:, :, None] == jnp.arange(expert_count, dtype=jnp.int32)[None, None, :]).astype(jnp.float32)
    coefficient = jnp.sum(hits * route_weight[:, :, None], axis=1)

    def add_expert(total, pieces):
        mid_piece, out_map, coef_column = pieces
        expert_out = jnp.dot(mid_piece, out_map, preferred_element_type=jnp.float32).astype(jnp.bfloat16)
        return total + coef_column[:, None] * expert_out.astype(jnp.float32), None

    adapter_sum, _ = lax.scan(add_expert, jnp.zeros((token_count, D), jnp.float32),
                              (jnp.transpose(rank_mid, (1, 0, 2)), adapter_out, coefficient.T))
    return (base_out + adapter_sum).astype(jnp.bfloat16)
```

```python
import functools

import jax
import jax.numpy as jnp
from jax import lax
from jax.experimental import pallas as pl
from jax.experimental.pallas import tpu as pltpu
from jax.sharding import PartitionSpec as P

LANES = 128
BF16 = jnp.bfloat16
F32 = jnp.float32
VM = pl.BlockSpec(memory_space=pltpu.VMEM)
HBM = pl.BlockSpec(memory_space=pltpu.HBM)
FLIP = (0, 2, 1, 3)


def in_hbm(x):
    return pltpu.with_memory_space_constraint(x, pltpu.HBM)


def params(mib):
    return pltpu.CompilerParams(vmem_limit_bytes=mib * 2**20)


def tile_copies(weight_ref, tiles_ref, sems, first):
    rows = 2 * weight_ref.shape[0]
    flat = weight_ref.reshape(rows, weight_ref.shape[2])
    return [
        pltpu.make_async_copy(
            flat.at[:, pl.ds((first + j) * LANES, LANES)], tiles_ref.at[j], sems.at[j]
        )
        for j in range(tiles_ref.shape[0])
    ]


def prep_kernel(
    tokens_in, ids_in, route_in, weight_ref, ext_ref, tiles_ref,
    tokens_ref, ids_ref, route_ref, own_sems, sems, *, first
):
    small = [
        pltpu.make_async_copy(source, target, own_sems.at[i])
        for i, (source, target) in enumerate(
            ((tokens_in, tokens_ref), (ids_in, ids_ref), (route_in, route_ref))
        )
    ]
    copies = tile_copies(weight_ref, tiles_ref, sems, first)
    for copy in small + copies:
        copy.start()
    for copy in small:
        copy.wait()
    top, rows = ids_ref.shape
    feat = tokens_ref.shape[1]
    number = lax.broadcasted_iota(jnp.int32, (LANES // 2, rows), 0)
    coef = jnp.zeros((LANES // 2, rows), F32)
    for k in range(top):
        coef = coef + jnp.where(ids_ref[k : k + 1, :] == number, route_ref[k : k + 1, :], 0.0)
    high = coef.astype(BF16)
    low = (coef - high.astype(F32)).astype(BF16)
    both = jnp.concatenate([high.astype(F32), low.astype(F32)], axis=0).astype(BF16)
    eye = (
        lax.broadcasted_iota(jnp.int32, (rows, rows), 0)
        == lax.broadcasted_iota(jnp.int32, (rows, rows), 1)
    ).astype(F32).astype(BF16)
    turned = lax.dot_general(eye, both, (((1,), (1,)), ((), ())), preferred_element_type=F32)
    ext_ref[:, :feat] = tokens_ref[...]
    ext_ref[:, feat:] = turned.astype(BF16)
    for copy in copies:
        copy.wait()


def load_kernel(weight_ref, tiles_ref, sems, *, first):
    copies = tile_copies(weight_ref, tiles_ref, sems, first)
    for copy in copies:
        copy.start()
    for copy in copies:
        copy.wait()


def pair_kernel(*refs, parts, feat):
    x_refs, refs = refs[:4], refs[4:]
    tile_refs, refs = refs[:parts], refs[parts:]
    in_ref, keep_ref, send_ref, all_ref, wide_ref = refs
    own = lax.axis_index("tp")
    rows = x_refs[0].shape[0]
    for s in range(4):
        all_ref[s] = x_refs[s][:, :feat]
    x = jnp.concatenate([all_ref[own ^ FLIP[i]] for i in range(4)], axis=0)
    half = 2 * rows
    rank = lax.dot_general(x, in_ref[...], (((1,), (1,)), ((), ())), preferred_element_type=F32)
    rank = jnp.concatenate([rank, jnp.zeros((4 * rows, LANES - rank.shape[1]), F32)], axis=1)
    spread = (
        2 * lax.broadcasted_iota(jnp.int32, (LANES, 2 * LANES), 0)
        == lax.broadcasted_iota(jnp.int32, (LANES, 2 * LANES), 1)
    ).astype(F32).astype(BF16)
    for b in range(feat // LANES):
        gate = jnp.dot(x[:, b * LANES : (b + 1) * LANES], spread, preferred_element_type=F32)
        up = pltpu.roll(gate, 1, 1).astype(BF16)
        gate = gate.astype(BF16)
        at = slice(2 * b * LANES, 2 * (b + 1) * LANES)
        wide_ref[0:half, at] = gate[:half]
        wide_ref[half : 2 * half, at] = up[:half]
        wide_ref[2 * half : 3 * half, at] = gate[half:]
        wide_ref[3 * half : 4 * half, at] = up[half:]
    width = (keep_ref.shape[1] - LANES) // 2
    keep_ref[:, 2 * width :] = rank[:half]
    send_ref[:, 2 * width :] = rank[half:].astype(BF16)
    at = 0
    for tiles_ref in tile_refs:
        count = tiles_ref.shape[0]
        for j in range(0, count, 2):
            n = min(2, count - j)
            weight = tiles_ref[j]
            if n == 2:
                weight = jnp.concatenate([weight, tiles_ref[j + 1]], axis=1)
            acc = jnp.dot(wide_ref[...], weight, preferred_element_type=F32)
            cols = slice(at, at + n * LANES)
            more = slice(width + at, width + at + n * LANES)
            keep_ref[:, cols] = acc[:half]
            keep_ref[:, more] = acc[half : 2 * half]
            send_ref[:, cols] = acc[2 * half : 3 * half].astype(BF16)
            send_ref[:, more] = acc[3 * half :].astype(BF16)
            at += n * LANES


def add_kernel(keep_ref, got_ref, mine_ref, send_ref):
    rows = mine_ref.shape[0]
    mine_ref[...] = keep_ref[:rows] + got_ref[:rows].astype(F32)
    send_ref[...] = (keep_ref[rows:] + got_ref[rows:].astype(F32)).astype(BF16)


def gate_kernel(mine_ref, got_ref, hidden_ref):
    width = (mine_ref.shape[1] - LANES) // 2
    gate = mine_ref[:, :width] + got_ref[:, :width].astype(F32)
    up = mine_ref[:, width : 2 * width] + got_ref[:, width : 2 * width].astype(F32)
    hidden_ref[:, :width] = (gate / (1.0 + jnp.exp(-gate)) * up).astype(BF16)
    hidden_ref[:, width:] = (mine_ref[:, 2 * width :] + got_ref[:, 2 * width :].astype(F32)).astype(BF16)


def down_kernel(*refs, feat, rank):
    h_refs, x_refs, (weight_ref, out_map_ref), o_refs, (turn_ref, all_ref) = (
        refs[:4], refs[4:8], refs[8:10], refs[10:14], refs[14:]
    )
    own = lax.axis_index("tp")
    expert = lax.axis_index("exp")
    rows = h_refs[0].shape[0]
    width = weight_ref.shape[0]
    for s in range(4):
        all_ref[s] = x_refs[s][:, feat:]
    hidden = jnp.concatenate([h[...] for h in h_refs], axis=0)
    acc = jnp.dot(hidden[:, :width], weight_ref[...], preferred_element_type=F32)
    lifted = jnp.dot(hidden[:, width : width + rank], out_map_ref[...], preferred_element_type=F32)
    lifted = lifted.astype(BF16).astype(F32)
    lane = lax.broadcasted_iota(jnp.int32, (4 * rows, LANES), 1)
    coef = jnp.concatenate([all_ref[own ^ FLIP[i]] for i in range(4)], axis=0).astype(F32)
    mine = (lane == expert) | (lane == expert + LANES // 2)
    coef = jnp.sum(jnp.where(mine, coef, 0.0), axis=1, keepdims=True)
    acc = acc + coef * lifted
    for i in range(4):
        turn_ref[own ^ FLIP[i]] = acc[i * rows : (i + 1) * rows]
    o_refs[0][...] = turn_ref[0]
    for s in range(1, 4):
        o_refs[s][...] = turn_ref[s].astype(BF16)


def swap(x, bit):
    return lax.ppermute(x, "tp", [(t, t ^ bit) for t in range(4)])


def fast(tokens, gate_up_weight, down_weight, adapter_in, adapter_out, expert_ids, route_weight):
    rows, feat = tokens.shape
    width = gate_up_weight.shape[2]
    rank = adapter_in.shape[2]
    count = width // LANES
    first = count // 2
    tiles = lambda n: pltpu.VMEM((n, 2 * feat, LANES), BF16)
    ext, tiles_a = pl.pallas_call(
        functools.partial(prep_kernel, first=0),
        out_shape=(jax.ShapeDtypeStruct((rows, feat + LANES), BF16), tiles(first)),
        in_specs=[HBM] * 4,
        out_specs=(VM, VM),
        scratch_shapes=[
            pltpu.VMEM((rows, feat), BF16),
            pltpu.VMEM(expert_ids.shape[::-1], jnp.int32),
            pltpu.VMEM(route_weight.shape[::-1], F32),
            pltpu.SemaphoreType.DMA((3,)),
            pltpu.SemaphoreType.DMA((first,)),
        ],
        compiler_params=params(2),
    )(*(in_hbm(a) for a in (tokens, expert_ids.T, route_weight.T, gate_up_weight)))
    xs = [ext] + [
        lax.ppermute(ext, "exp", [(e, (e + s) % 4) for e in range(4)]) for s in range(1, 4)
    ]
    tiles_b = pl.pallas_call(
        functools.partial(load_kernel, first=first),
        out_shape=tiles(count - first),
        in_specs=[HBM],
        out_specs=VM,
        scratch_shapes=[pltpu.SemaphoreType.DMA((count - first,))],
        compiler_params=params(2),
    )(in_hbm(gate_up_weight))
    total = 2 * width + LANES
    shape = jax.ShapeDtypeStruct
    keep, send = pl.pallas_call(
        functools.partial(pair_kernel, parts=2, feat=feat),
        out_shape=(shape((2 * rows, total), F32), shape((2 * rows, total), BF16)),
        in_specs=[VM] * 7,
        out_specs=(VM, VM),
        scratch_shapes=[pltpu.VMEM((4, rows, feat), BF16), pltpu.VMEM((8 * rows, 2 * feat), BF16)],
        compiler_params=params(8),
    )(*xs, tiles_a, tiles_b, jnp.swapaxes(adapter_in, 1, 2)[0])
    got = swap(send, 1)
    mine, send = pl.pallas_call(
        add_kernel,
        out_shape=(shape((rows, total), F32), shape((rows, total), BF16)),
        in_specs=[VM, VM],
        out_specs=(VM, VM),
        compiler_params=params(4),
    )(keep, got)
    got = swap(send, 2)
    hidden = pl.pallas_call(
        gate_kernel,
        out_shape=shape((rows, width + LANES), BF16),
        in_specs=[VM, VM],
        out_specs=VM,
        compiler_params=params(4),
    )(mine, got)
    far = swap(hidden, 2)
    hs = [hidden, far, swap(hidden, 1), swap(far, 1)]
    outs = pl.pallas_call(
        functools.partial(down_kernel, feat=feat, rank=rank),
        out_shape=[shape((rows, feat), F32)] + [shape((rows, feat), BF16)] * 3,
        in_specs=[VM] * 10,
        out_specs=[VM] * 4,
        scratch_shapes=[pltpu.VMEM((4, rows, feat), F32), pltpu.VMEM((4, rows, LANES), BF16)],
        compiler_params=params(16),
    )(*hs, *xs, down_weight, adapter_out[0])
    total = outs[0]
    for s in range(1, 4):
        back = lax.ppermute(outs[s], "exp", [(e, (e - s) % 4) for e in range(4)])
        total = total + back.astype(F32)
    return total.astype(BF16)


def plain(tokens, gate_up_weight, down_weight, adapter_in, adapter_out, expert_ids, route_weight):
    exp_count = lax.axis_size("exp")
    own_rows, feat_width = tokens.shape
    all_tokens = lax.all_gather(tokens, "exp", axis=0, tiled=True)
    hidden_width = gate_up_weight.shape[2]
    pair_weight = gate_up_weight.reshape(feat_width, 2 * hidden_width)
    pair_share = lax.psum_scatter(
        jnp.dot(all_tokens, pair_weight, preferred_element_type=jnp.float32).astype(jnp.bfloat16),
        "tp",
        scatter_dimension=0,
        tiled=True,
    ).astype(jnp.float32)
    hidden_share = (
        jax.nn.silu(pair_share[:, :hidden_width]) * pair_share[:, hidden_width:]
    ).astype(jnp.bfloat16)
    hidden = lax.all_gather(hidden_share, "tp", axis=0, tiled=True)
    base_out = lax.psum_scatter(
        jnp.dot(hidden, down_weight, preferred_element_type=jnp.float32).astype(jnp.bfloat16),
        "exp",
        scatter_dimension=0,
        tiled=True,
    ).astype(jnp.float32)
    top_count = expert_ids.shape[1]
    expert_count = adapter_in.shape[0] * exp_count
    flat_ids = expert_ids.reshape(own_rows * top_count)
    flat_weight = route_weight.reshape(own_rows * top_count)
    expert_hits = (flat_ids[:, None] == jnp.arange(expert_count, dtype=jnp.int32)[None, :]).astype(
        jnp.int32
    )
    capacity = max(2, 2 * top_count * own_rows // expert_count)
    slot_index = jnp.sum((jnp.cumsum(expert_hits, axis=0) - expert_hits) * expert_hits, axis=1)
    slot_target = flat_ids * capacity + slot_index
    slot_hits = (
        slot_target[:, None] == jnp.arange(expert_count * capacity, dtype=jnp.int32)[None, :]
    )
    combine_matrix = jnp.sum(
        (slot_hits.astype(jnp.float32) * flat_weight[:, None]).reshape(
            own_rows, top_count, expert_count * capacity
        ),
        axis=1,
    )
    dispatch_matrix = slot_hits.T.astype(jnp.bfloat16)
    repeated = jnp.repeat(tokens, top_count, axis=0)
    outgoing = jnp.dot(dispatch_matrix, repeated, preferred_element_type=jnp.float32).astype(
        jnp.bfloat16
    )
    outgoing = outgoing.reshape(expert_count, capacity, feat_width)
    rank_partial = jnp.einsum(
        "scd,dr->scr",
        lax.all_to_all(outgoing, "exp", split_axis=0, concat_axis=0, tiled=True),
        adapter_in[0],
        preferred_element_type=jnp.float32,
    )
    rank_mid = lax.psum(rank_partial, "tp").astype(jnp.bfloat16)
    expert_out = jnp.einsum(
        "scr,rd->scd", rank_mid, adapter_out[0], preferred_element_type=jnp.float32
    ).astype(jnp.bfloat16)
    returned = lax.all_to_all(expert_out, "exp", split_axis=0, concat_axis=0, tiled=True)
    adapter_sum = jnp.dot(
        combine_matrix,
        returned.reshape(expert_count * capacity, feat_width).astype(jnp.float32),
        precision=lax.Precision.HIGHEST,
        preferred_element_type=jnp.float32,
    )
    return (base_out + adapter_sum).astype(jnp.bfloat16)


def solution(mesh):
    in_specs = (
        P(("grp", "exp"), "tp"),
        P("tp", None, "exp"),
        P("exp", "tp"),
        P("exp", "tp", None),
        P("exp", None, "tp"),
        P(("grp", "exp"), None),
        P(("grp", "exp"), None),
    )
    out_specs = P(("grp", "exp"), "tp")
    def local(*args):
        rows, feat = args[0].shape
        width = args[1].shape[2]
        aligned = feat % LANES == 0 and width % LANES == 0 and rows % 16 == 0
        few = args[3].shape[0] == 1 and mesh.shape["exp"] <= LANES // 2
        square = mesh.shape["tp"] == 4 and mesh.shape["exp"] == 4
        return (fast if aligned and few and square else plain)(*args)

    return jax.shard_map(local, mesh=mesh, in_specs=in_specs, out_specs=out_specs, check_vma=False)
```

```python
import functools

import jax
import jax.numpy as jnp
from jax import lax
from jax.experimental import pallas as pl
from jax.experimental.pallas import tpu as pltpu
from jax.sharding import PartitionSpec as P


LANES = 128
BF16 = jnp.bfloat16
F32 = jnp.float32
VM = pl.BlockSpec(memory_space=pltpu.VMEM)
HBM = pl.BlockSpec(memory_space=pltpu.HBM)
FLIP = (0, 2, 1, 3)


def in_hbm(x):
    return pltpu.with_memory_space_constraint(x, pltpu.HBM)


def params(mib):
    return pltpu.CompilerParams(vmem_limit_bytes=mib * 2**20)


def tile_copies(weight_ref, tiles_ref, sems, first):
    rows = 2 * weight_ref.shape[0]
    flat = weight_ref.reshape(rows, weight_ref.shape[2])
    return [
        pltpu.make_async_copy(
            flat.at[:, pl.ds((first + j) * LANES, LANES)], tiles_ref.at[j], sems.at[j]
        )
        for j in range(tiles_ref.shape[0])
    ]


def prep_kernel(
    tokens_in, ids_in, route_in, weight_ref, ext_ref, tiles_ref,
    tokens_ref, ids_ref, route_ref, own_sems, sems, *, first
):
    small = [
        pltpu.make_async_copy(source, target, own_sems.at[i])
        for i, (source, target) in enumerate(
            ((tokens_in, tokens_ref), (ids_in, ids_ref), (route_in, route_ref))
        )
    ]
    copies = tile_copies(weight_ref, tiles_ref, sems, first)
    for copy in small + copies:
        copy.start()
    for copy in small:
        copy.wait()
    top, rows = ids_ref.shape
    feat = tokens_ref.shape[1]
    number = lax.broadcasted_iota(jnp.int32, (LANES // 2, rows), 0)
    coef = jnp.zeros((LANES // 2, rows), F32)
    for k in range(top):
        coef = coef + jnp.where(ids_ref[k : k + 1, :] == number, route_ref[k : k + 1, :], 0.0)
    high = coef.astype(BF16)
    low = (coef - high.astype(F32)).astype(BF16)
    both = jnp.concatenate([high.astype(F32), low.astype(F32)], axis=0).astype(BF16)
    eye = (
        lax.broadcasted_iota(jnp.int32, (rows, rows), 0)
        == lax.broadcasted_iota(jnp.int32, (rows, rows), 1)
    ).astype(F32).astype(BF16)
    turned = lax.dot_general(eye, both, (((1,), (1,)), ((), ())), preferred_element_type=F32)
    ext_ref[:, :feat] = tokens_ref[...]
    ext_ref[:, feat:] = turned.astype(BF16)
    for copy in copies:
        copy.wait()


def load_kernel(weight_ref, tiles_ref, sems, *, first):
    copies = tile_copies(weight_ref, tiles_ref, sems, first)
    for copy in copies:
        copy.start()
    for copy in copies:
        copy.wait()


def products(wide_ref, tile_refs, keep_ref, send_ref, width):
    half = keep_ref.shape[0]
    tiles = [(ref, j) for ref in tile_refs for j in range(ref.shape[0])]
    for at in range(0, len(tiles), 2):
        group = [ref[j] for ref, j in tiles[at : at + 2]]
        weight = group[0] if len(group) == 1 else jnp.concatenate(group, axis=1)
        acc = jnp.dot(wide_ref[...], weight, preferred_element_type=F32)
        cols = slice(at * LANES, (at + len(group)) * LANES)
        more = slice(width + cols.start, width + cols.stop)
        keep_ref[:, cols] = acc[:half]
        keep_ref[:, more] = acc[half : 2 * half]
        send_ref[:, cols] = acc[2 * half : 3 * half].astype(BF16)
        send_ref[:, more] = acc[3 * half :].astype(BF16)


def first_pair_kernel(
    x0_ref, x1_ref, x2_ref, x3_ref, now_ref, in_ref, weight_ref,
    keep_ref, send_ref, wide_ref, late_ref, all_ref, sems, *, feat, first
):
    copies = tile_copies(weight_ref, late_ref, sems, first)
    for copy in copies:
        copy.start()
    own = lax.axis_index("tp")
    rows = x0_ref.shape[0]
    for s, ref in enumerate((x0_ref, x1_ref, x2_ref, x3_ref)):
        all_ref[s] = ref[:, :feat]
    x = jnp.concatenate([all_ref[own ^ FLIP[i]] for i in range(4)], axis=0)
    half = 2 * rows
    spread = (
        2 * lax.broadcasted_iota(jnp.int32, (LANES, 2 * LANES), 0)
        == lax.broadcasted_iota(jnp.int32, (LANES, 2 * LANES), 1)
    ).astype(F32).astype(BF16)
    for b in range(feat // LANES):
        gate = jnp.dot(x[:, b * LANES : (b + 1) * LANES], spread, preferred_element_type=F32)
        up = pltpu.roll(gate, 1, 1).astype(BF16)
        gate = gate.astype(BF16)
        at = slice(2 * b * LANES, 2 * (b + 1) * LANES)
        wide_ref[0:half, at] = gate[:half]
        wide_ref[half : 2 * half, at] = up[:half]
        wide_ref[2 * half : 3 * half, at] = gate[half:]
        wide_ref[3 * half : 4 * half, at] = up[half:]
    rank = lax.dot_general(x, in_ref[...], (((1,), (1,)), ((), ())), preferred_element_type=F32)
    rank = jnp.concatenate([rank, jnp.zeros((4 * rows, LANES - rank.shape[1]), F32)], axis=1)
    width = (keep_ref.shape[1] - LANES) // 2
    keep_ref[:, 2 * width :] = rank[:half]
    send_ref[:, 2 * width :] = rank[half:].astype(BF16)
    products(wide_ref, [now_ref], keep_ref, send_ref, width)
    for copy in copies:
        copy.wait()


def second_pair_kernel(wide_ref, early_ref, late_ref, keep_ref, send_ref):
    products(wide_ref, [early_ref, late_ref], keep_ref, send_ref, keep_ref.shape[1] // 2)


def add_kernel(keep_ref, got_ref, mine_ref, send_ref):
    rows = mine_ref.shape[0]
    mine_ref[...] = keep_ref[:rows] + got_ref[:rows].astype(F32)
    send_ref[...] = (keep_ref[rows:] + got_ref[rows:].astype(F32)).astype(BF16)


def gate_kernel(mine_ref, got_ref, hidden_ref, *, width):
    gate = mine_ref[:, :width] + got_ref[:, :width].astype(F32)
    up = mine_ref[:, width : 2 * width] + got_ref[:, width : 2 * width].astype(F32)
    hidden_ref[:, :width] = (gate / (1.0 + jnp.exp(-gate)) * up).astype(BF16)
    if hidden_ref.shape[1] > width:
        rank = mine_ref[:, 2 * width :] + got_ref[:, 2 * width :].astype(F32)
        hidden_ref[:, width:] = rank.astype(BF16)


def first_down_kernel(*refs, feat, rank):
    h_refs, x_refs, (weight_ref, out_map_ref, acc_ref, all_ref) = refs[:4], refs[4:8], refs[8:]
    own = lax.axis_index("tp")
    expert = lax.axis_index("exp")
    rows = h_refs[0].shape[0]
    width = h_refs[0].shape[1] - LANES
    for s in range(4):
        all_ref[s] = x_refs[s][:, feat:]
    hidden = jnp.concatenate([h[...] for h in h_refs], axis=0)
    acc = jnp.dot(hidden[:, :width], weight_ref[:width], preferred_element_type=F32)
    lifted = jnp.dot(hidden[:, width : width + rank], out_map_ref[...], preferred_element_type=F32)
    lifted = lifted.astype(BF16).astype(F32)
    lane = lax.broadcasted_iota(jnp.int32, (4 * rows, LANES), 1)
    coef = jnp.concatenate([all_ref[own ^ FLIP[i]] for i in range(4)], axis=0).astype(F32)
    mine = (lane == expert) | (lane == expert + LANES // 2)
    coef = jnp.sum(jnp.where(mine, coef, 0.0), axis=1, keepdims=True)
    acc_ref[...] = acc + coef * lifted


def second_down_kernel(h0_ref, h1_ref, h2_ref, h3_ref, weight_ref, first_ref, *o_refs):
    o_refs, turn_ref = o_refs[:4], o_refs[4]
    own = lax.axis_index("tp")
    rows, width = h0_ref.shape
    hidden = jnp.concatenate([h[...] for h in (h0_ref, h1_ref, h2_ref, h3_ref)], axis=0)
    acc = first_ref[...] + jnp.dot(
        hidden, weight_ref[weight_ref.shape[0] - width :], preferred_element_type=F32
    )
    for i in range(4):
        turn_ref[own ^ FLIP[i]] = acc[i * rows : (i + 1) * rows]
    o_refs[0][...] = turn_ref[0]
    for s in range(1, 4):
        o_refs[s][...] = turn_ref[s].astype(BF16)


def swap(x, bit):
    return lax.ppermute(x, "tp", [(t, t ^ bit) for t in range(4)])


def fast(tokens, gate_up_weight, down_weight, adapter_in, adapter_out, expert_ids, route_weight):
    rows, feat = tokens.shape
    width = gate_up_weight.shape[2]
    rank = adapter_in.shape[2]
    count = width // LANES
    first = count // 2
    tiles = lambda n: pltpu.VMEM((n, 2 * feat, LANES), BF16)
    ext, tiles_a = pl.pallas_call(
        functools.partial(prep_kernel, first=0),
        out_shape=(jax.ShapeDtypeStruct((rows, feat + LANES), BF16), tiles(first)),
        in_specs=[HBM] * 4,
        out_specs=(VM, VM),
        scratch_shapes=[
            pltpu.VMEM((rows, feat), BF16),
            pltpu.VMEM(expert_ids.shape[::-1], jnp.int32),
            pltpu.VMEM(route_weight.shape[::-1], F32),
            pltpu.SemaphoreType.DMA((3,)),
            pltpu.SemaphoreType.DMA((first,)),
        ],
        compiler_params=params(2),
    )(*(in_hbm(a) for a in (tokens, expert_ids.T, route_weight.T, gate_up_weight)))
    xs = [ext]
    for s in range(1, 4):
        xs.append(lax.ppermute(ext, "exp", [(e, e ^ s) for e in range(4)]))
    late = (count - first) // 3
    early = count - first - late
    tiles_b = pl.pallas_call(
        functools.partial(load_kernel, first=first),
        out_shape=tiles(early),
        in_specs=[HBM],
        out_specs=VM,
        scratch_shapes=[pltpu.SemaphoreType.DMA((early,))],
        compiler_params=params(2),
    )(in_hbm(gate_up_weight))
    shape = jax.ShapeDtypeStruct
    total_a = 2 * first * LANES + LANES
    total_b = 2 * (count - first) * LANES
    keep_a, send_a, wide, tiles_c = pl.pallas_call(
        functools.partial(first_pair_kernel, feat=feat, first=first + early),
        out_shape=(
            shape((2 * rows, total_a), F32),
            shape((2 * rows, total_a), BF16),
            pltpu.VMEM((8 * rows, 2 * feat), BF16),
            tiles(late),
        ),
        in_specs=[VM] * 6 + [HBM],
        out_specs=(VM,) * 4,
        scratch_shapes=[pltpu.VMEM((4, rows, feat), BF16), pltpu.SemaphoreType.DMA((late,))],
        compiler_params=params(6),
    )(*xs, tiles_a, jnp.swapaxes(adapter_in, 1, 2)[0], in_hbm(gate_up_weight))
    got_a = swap(send_a, 1)
    keep_b, send_b = pl.pallas_call(
        second_pair_kernel,
        out_shape=(shape((2 * rows, total_b), F32), shape((2 * rows, total_b), BF16)),
        in_specs=[VM] * 3,
        out_specs=(VM, VM),
        compiler_params=params(6),
    )(wide, tiles_b, tiles_c)
    got_b = swap(send_b, 1)

    def add(keep, got):
        return pl.pallas_call(
            add_kernel,
            out_shape=(shape((rows, keep.shape[1]), F32), shape((rows, keep.shape[1]), BF16)),
            in_specs=[VM, VM],
            out_specs=(VM, VM),
            compiler_params=params(4),
        )(keep, got)

    def gate(mine, got, columns):
        return pl.pallas_call(
            functools.partial(gate_kernel, width=columns),
            out_shape=shape((rows, mine.shape[1] - columns), BF16),
            in_specs=[VM, VM],
            out_specs=VM,
            compiler_params=params(4),
        )(mine, got)

    mine_a, send_a = add(keep_a, got_a)
    got_a = swap(send_a, 2)
    mine_b, send_b = add(keep_b, got_b)
    got_b = swap(send_b, 2)
    hidden_a = gate(mine_a, got_a, first * LANES)
    far_a = swap(hidden_a, 2)
    near_a = swap(hidden_a, 1)
    hidden_b = gate(mine_b, got_b, (count - first) * LANES)
    far_b = swap(hidden_b, 2)
    near_b = swap(hidden_b, 1)
    acc = pl.pallas_call(
        functools.partial(first_down_kernel, feat=feat, rank=rank),
        out_shape=shape((4 * rows, feat), F32),
        in_specs=[VM] * 10,
        out_specs=VM,
        scratch_shapes=[pltpu.VMEM((4, rows, LANES), BF16)],
        compiler_params=params(8),
    )(hidden_a, far_a, near_a, swap(far_a, 1), *xs, down_weight, adapter_out[0])
    outs = pl.pallas_call(
        second_down_kernel,
        out_shape=[shape((rows, feat), F32)] + [shape((rows, feat), BF16)] * 3,
        in_specs=[VM] * 6,
        out_specs=[VM] * 4,
        scratch_shapes=[pltpu.VMEM((4, rows, feat), F32)],
        compiler_params=params(8),
    )(hidden_b, far_b, near_b, swap(far_b, 1), down_weight, acc)
    total = outs[0]
    for s in range(1, 4):
        back = lax.ppermute(outs[s], "exp", [(e, e ^ s) for e in range(4)])
        total = total + back.astype(F32)
    return total.astype(BF16)


def plain(tokens, gate_up_weight, down_weight, adapter_in, adapter_out, expert_ids, route_weight):
    exp_count = lax.axis_size("exp")
    own_rows, feat_width = tokens.shape
    all_tokens = lax.all_gather(tokens, "exp", axis=0, tiled=True)
    hidden_width = gate_up_weight.shape[2]
    pair_weight = gate_up_weight.reshape(feat_width, 2 * hidden_width)
    pair_share = lax.psum_scatter(
        jnp.dot(all_tokens, pair_weight, preferred_element_type=jnp.float32).astype(jnp.bfloat16),
        "tp",
        scatter_dimension=0,
        tiled=True,
    ).astype(jnp.float32)
    hidden_share = (
        jax.nn.silu(pair_share[:, :hidden_width]) * pair_share[:, hidden_width:]
    ).astype(jnp.bfloat16)
    hidden = lax.all_gather(hidden_share, "tp", axis=0, tiled=True)
    base_out = lax.psum_scatter(
        jnp.dot(hidden, down_weight, preferred_element_type=jnp.float32).astype(jnp.bfloat16),
        "exp",
        scatter_dimension=0,
        tiled=True,
    ).astype(jnp.float32)
    top_count = expert_ids.shape[1]
    expert_count = adapter_in.shape[0] * exp_count
    flat_ids = expert_ids.reshape(own_rows * top_count)
    flat_weight = route_weight.reshape(own_rows * top_count)
    expert_hits = (flat_ids[:, None] == jnp.arange(expert_count, dtype=jnp.int32)[None, :]).astype(
        jnp.int32
    )
    capacity = max(2, 2 * top_count * own_rows // expert_count)
    slot_index = jnp.sum((jnp.cumsum(expert_hits, axis=0) - expert_hits) * expert_hits, axis=1)
    slot_target = flat_ids * capacity + slot_index
    slot_hits = (
        slot_target[:, None] == jnp.arange(expert_count * capacity, dtype=jnp.int32)[None, :]
    )
    combine_matrix = jnp.sum(
        (slot_hits.astype(jnp.float32) * flat_weight[:, None]).reshape(
            own_rows, top_count, expert_count * capacity
        ),
        axis=1,
    )
    dispatch_matrix = slot_hits.T.astype(jnp.bfloat16)
    repeated = jnp.repeat(tokens, top_count, axis=0)
    outgoing = jnp.dot(dispatch_matrix, repeated, preferred_element_type=jnp.float32).astype(
        jnp.bfloat16
    )
    outgoing = outgoing.reshape(expert_count, capacity, feat_width)
    rank_partial = jnp.einsum(
        "scd,dr->scr",
        lax.all_to_all(outgoing, "exp", split_axis=0, concat_axis=0, tiled=True),
        adapter_in[0],
        preferred_element_type=jnp.float32,
    )
    rank_mid = lax.psum(rank_partial, "tp").astype(jnp.bfloat16)
    expert_out = jnp.einsum(
        "scr,rd->scd", rank_mid, adapter_out[0], preferred_element_type=jnp.float32
    ).astype(jnp.bfloat16)
    returned = lax.all_to_all(expert_out, "exp", split_axis=0, concat_axis=0, tiled=True)
    adapter_sum = jnp.dot(
        combine_matrix,
        returned.reshape(expert_count * capacity, feat_width).astype(jnp.float32),
        precision=lax.Precision.HIGHEST,
        preferred_element_type=jnp.float32,
    )
    return (base_out + adapter_sum).astype(jnp.bfloat16)


def solution(mesh):
    in_specs = (
        P(("grp", "exp"), "tp"),
        P("tp", None, "exp"),
        P("exp", "tp"),
        P("exp", "tp", None),
        P("exp", None, "tp"),
        P(("grp", "exp"), None),
        P(("grp", "exp"), None),
    )
    out_specs = P(("grp", "exp"), "tp")

    def local(*args):
        rows, feat = args[0].shape
        width = args[1].shape[2]
        aligned = feat % LANES == 0 and width % LANES == 0 and rows % 16 == 0
        few = args[3].shape[0] == 1 and mesh.shape["exp"] <= LANES // 2
        square = mesh.shape["tp"] == 4 and mesh.shape["exp"] == 4
        if not (aligned and few and square):
            return plain(*args)
        return fast(*args)

    return jax.shard_map(local, mesh=mesh, in_specs=in_specs, out_specs=out_specs, check_vma=False)
```
